32 devices in a mesh: tensor: 4 (over z), dp: 8 (over y, x, core).
Axes of the slice: x: 2, y: 2, z: 4, core: 2. Of those that a mesh axis runs over, the one named last changes fastest.
Arguments:
- grads: bfloat16 [8, 40, 28672], P('dp', None, 'tensor'), may hold values from -6 to 6
- offload_mask: int32 [8, 5], replicated, may hold values from 0 to 1, as said below
- owner_map: int32 [8], replicated, may hold values from 0 to 7, as said below
- local_master: float32 [24, 28672], P('dp', 'tensor'), may hold values from -6 to 6
- local_moment: float32 [24, 28672], P('dp', 'tensor'), may hold values from -1.2 to 1.2
- local_second: float32 [24, 28672], P('dp', 'tensor'), may hold values from 0.001 to 0.1
- offload_master: float32 [16, 2, 28672], P('dp', None, 'tensor'), may hold values from -6 to 6
- offload_moment: float32 [16, 2, 28672], P('dp', None, 'tensor'), may hold values from -1.2 to 1.2
- offload_second: float32 [16, 2, 28672], P('dp', None, 'tensor'), may hold values from 0.001 to 0.1
Outputs:
- new_weights: bfloat16 [40, 28672], P(None, 'tensor')
- grad_norm: float32 [], replicated
- new_local_master: float32 [24, 28672], P('dp', 'tensor')
- new_local_moment: float32 [24, 28672], P('dp', 'tensor')
- new_local_second: float32 [24, 28672], P('dp', 'tensor')
- new_offload_master: float32 [16, 2, 28672], P('dp', None, 'tensor')
- new_offload_moment: float32 [16, 2, 28672], P('dp', None, 'tensor')
- new_offload_second: float32 [16, 2, 28672], P('dp', None, 'tensor')
The draws below stay inside these ranges and needn't reach their ends.
Inputs may be any that keep to these rules, and one draw needn't show every extreme that they name: Each row of offload_mask holds exactly 2 ones. `owner_map`: no device is named by more than 2 shards, and some device is named by exactly 2.
All inputs are finite; a program needn't handle non-finite values.
Results may differ from the reference program's by a relative error of at most 0.0039.
Values may be sent and summed in bfloat16 or wider, within the bound.
A program may use at most 128 MiB of HBM per device.

```python
import math
import jax
import jax.numpy as jnp
from jax import lax

FF = 28672
ROW_DEV = 5
SLOTS = 2
OFF = 2
KEEP = 3
ROWS = 40
N_DP = 8


def draw_offload_mask(key, part):
    scores = jax.random.randint(key, (N_DP, ROW_DEV), 0, 1 << 20) * ROW_DEV + jnp.arange(ROW_DEV, dtype=jnp.int32)[None, :]
    ordering = jnp.argsort(scores, axis=1, stable=True)
    ranking = jnp.argsort(ordering, axis=1, stable=True)
    return (ranking < OFF).astype(jnp.int32)


def draw_owner_map(key, part):
    shard_numbers = jnp.arange(N_DP, dtype=jnp.int32)
    chosen = jax.random.randint(jax.random.fold_in(key, 7), (), 0, N_DP).astype(jnp.int32)
    opposite = (shard_numbers + N_DP // 2) % N_DP
    forward_shard = chosen
    backward_shard = (chosen + 3) % N_DP
    owners = jnp.where(shard_numbers == forward_shard, (chosen + 1) % N_DP, opposite)
    owners = jnp.where(shard_numbers == backward_shard, (chosen + 2) % N_DP, owners)
    return owners.astype(jnp.int32)


def strengthened(entries, own_key, source, target, shards_of, factor):
    owner, partner = [(jnp.arange(entries.shape[axis_at]) // (entries.shape[axis_at] // shards_of)).reshape([-1 if axis == axis_at else 1 for axis in range(entries.ndim)]) for axis_at in (source, target)]
    chosen = jax.random.permutation(own_key, shards_of)[partner]
    strong = (owner == chosen) | (owner == (partner + shards_of // 2) % shards_of)
    return jnp.where(strong, factor * entries, entries)


def level_of(stream_key, shape, pieces, smallest, top_value):
    def one(dim, blocks):
        draws = jax.random.uniform(jax.random.fold_in(jax.random.fold_in(stream_key, 6), dim), (blocks,), jnp.float32, smallest / len(pieces), top_value / len(pieces))
        return jnp.repeat(jnp.exp(draws), shape[dim] // blocks).reshape((-1,) + (1,) * (len(shape) - dim - 1))

    factor_of = one(*pieces[0])
    for cut in pieces[1:]:
        factor_of = factor_of * one(*cut)
    return factor_of


def noise(stream_key, dims, spread, most, cuts=(), kind=jnp.bfloat16):
    level = level_of(stream_key, dims, cuts, -0.22, 0.18) if cuts else 1.0
    result = jax.random.normal(stream_key, dims, jnp.float32) * spread * level
    return jnp.minimum(jnp.maximum(result, -most), most).astype(kind)


def bell_draw_with(own_key, extent, scale, reach, cuts, heavy, kind=jnp.bfloat16):
    values = scale * jax.random.normal(own_key, extent, jnp.float32)
    if cuts:
        values = values * level_of(own_key, extent, cuts, -0.22, 0.18)
    return jnp.clip(strengthened(values, jax.random.fold_in(own_key, 3), *heavy), -reach, reach).astype(kind)


def setup_inputs(seed: int = 0) -> dict:
    arg_keys = jax.random.split(jax.random.key(seed), 10)
    grads = bell_draw_with(arg_keys[0], (N_DP, ROWS, FF), 1.0, 6.0, ((0, 8), (2, 4)), (0, 1, 8, 2.0))
    offload_mask = draw_offload_mask(jax.random.fold_in(arg_keys[9], 71), 0)
    owner_map = draw_owner_map(jax.random.fold_in(arg_keys[9], 71), 0)
    local_master = noise(arg_keys[3], (N_DP * KEEP, FF), 1.0, 6.0, ((0, 8), (1, 4)), jnp.float32)
    local_moment = noise(arg_keys[4], (N_DP * KEEP, FF), 0.2, 1.2, ((0, 8), (1, 4)), jnp.float32)
    local_second = jnp.clip(jnp.exp(math.log(0.1) - 4.6051702 * jax.random.uniform(arg_keys[5], (N_DP * KEEP, FF), jnp.float32) ** level_of(arg_keys[5], (N_DP * KEEP, FF), ((0, 8), (1, 4)), -0.2, 0.2)), 0.001, 0.1)
    offload_master = noise(arg_keys[6], (N_DP * SLOTS, OFF, FF), 1.0, 6.0, ((0, 8), (2, 4)), jnp.float32)
    offload_moment = noise(arg_keys[7], (N_DP * SLOTS, OFF, FF), 0.2, 1.2, ((0, 8), (2, 4)), jnp.float32)
    offload_second = jnp.clip(jnp.exp(math.log(0.1) - 4.6051702 * jax.random.uniform(arg_keys[8], (N_DP * SLOTS, OFF, FF), jnp.float32) ** level_of(arg_keys[8], (N_DP * SLOTS, OFF, FF), ((0, 8), (2, 4)), -0.2, 0.2)), 0.001, 0.1)
    return {"grads": grads, "offload_mask": offload_mask, "owner_map": owner_map, "local_master": local_master, "local_moment": local_moment, "local_second": local_second, "offload_master": offload_master, "offload_moment": offload_moment, "offload_second": offload_second}


beta_first = 0.9
beta_second = 0.95
learn_rate = 0.02
decay_rate = 0.1
epsilon_value = 1e-08
step_count = 10
bias_first = 1.0 - beta_first ** step_count
bias_second = 1.0 - beta_second ** step_count

def adam_update(master, moment, second, gradient):
    moment_new = beta_first * moment + (1.0 - beta_first) * gradient
    second_new = beta_second * second + (1.0 - beta_second) * gradient * gradient
    scaled = moment_new / bias_first / (jnp.sqrt(second_new / bias_second) + epsilon_value)
    master_new = master - learn_rate * (scaled + decay_rate * master)
    return (master_new, moment_new, second_new)

def row_tables(offload_mask, owner_map):
    shards = owner_map.shape[0]
    row_dev = offload_mask.shape[1]
    numbers = jnp.arange(shards, dtype=jnp.int32)
    same_owner = owner_map[:, None] == owner_map[None, :]
    earlier = numbers[None, :] < numbers[:, None]
    slot_of = lax.optimization_barrier(jnp.sum((same_owner & earlier).astype(jnp.int32), axis=1))
    off_rank = (jnp.cumsum(offload_mask, axis=1) - offload_mask).astype(jnp.int32)
    keep_rank = jnp.arange(row_dev, dtype=jnp.int32)[None, :] - off_rank
    return (slot_of, off_rank, keep_rank)

def reference(grads, offload_mask, owner_map, local_master, local_moment, local_second, offload_master, offload_moment, offload_second):

    def accumulate(member, running):
        return running + grads[member].astype(jnp.float32)
    summed = lax.fori_loop(0, N_DP, accumulate, jnp.zeros((ROWS, FF), jnp.float32))
    gradient = summed / N_DP
    grad_norm = jnp.sqrt(jnp.sum(gradient * gradient))
    slot_of, off_rank, keep_rank = row_tables(offload_mask, owner_map)
    shard_ids = jnp.arange(N_DP, dtype=jnp.int32)[:, None]
    row_ids = (shard_ids * ROW_DEV + jnp.arange(ROW_DEV, dtype=jnp.int32)[None, :]).reshape(-1)
    is_off = (offload_mask == 1).reshape(-1)
    local_pos = (shard_ids * KEEP + keep_rank).reshape(-1).astype(jnp.int32)
    entry_pos = ((owner_map * SLOTS + slot_of)[:, None] * OFF + off_rank).reshape(-1).astype(jnp.int32)
    keep_row_of = jnp.zeros((N_DP * KEEP,), jnp.int32).at[jnp.where(is_off, N_DP * KEEP, local_pos)].set(row_ids, mode='drop')
    off_row_of = jnp.full((N_DP * SLOTS * OFF,), -1, jnp.int32).at[jnp.where(is_off, entry_pos, N_DP * SLOTS * OFF)].set(row_ids, mode='drop')
    filled = (off_row_of >= 0).reshape(N_DP * SLOTS, OFF, 1)
    new_local = adam_update(local_master, local_moment, local_second, jnp.take(gradient, keep_row_of, axis=0))
    off_grad = jnp.take(gradient, jnp.maximum(off_row_of, 0), axis=0).reshape(N_DP * SLOTS, OFF, FF)
    updated = adam_update(offload_master, offload_moment, offload_second, off_grad)
    formers = (offload_master, offload_moment, offload_second)
    new_off = tuple((jnp.where(filled, updated[place], formers[place]) for place in range(3)))
    from_local = jnp.take(new_local[0], jnp.where(is_off, 0, local_pos), axis=0)
    from_off = jnp.take(new_off[0].reshape(N_DP * SLOTS * OFF, FF), jnp.where(is_off, entry_pos, 0), axis=0)
    new_weights = jnp.where(is_off[:, None], from_off, from_local).astype(jnp.bfloat16)
    return (new_weights, grad_norm, new_local[0], new_local[1], new_local[2], new_off[0], new_off[1], new_off[2])
```

```python
import functools

import jax
import jax.numpy as jnp
from jax import lax
from jax.experimental import pallas as pl
from jax.experimental.pallas import tpu as pltpu
from jax.sharding import PartitionSpec as P

MESH = pl.DeviceIdType.MESH
beta_first = 0.9
beta_second = 0.95
learn_rate = 0.02
decay_rate = 0.1
epsilon_value = 1e-08
step_count = 10
bias_first = 1.0 - beta_first**step_count
bias_second = 1.0 - beta_second**step_count
LANES = 128
SUBLANES = 8


def adam_update(master, moment, second, gradient):
    moment_new = beta_first * moment + (1.0 - beta_first) * gradient
    second_new = beta_second * second + (1.0 - beta_second) * gradient * gradient
    scaled = moment_new / bias_first / (jnp.sqrt(second_new / bias_second) + epsilon_value)
    master_new = master - learn_rate * (scaled + decay_rate * master)
    return (master_new, moment_new, second_new)


def kernel(
    n,
    tensors,
    chunks,
    mask_ref,
    owner_ref,
    grads,
    lm_in,
    l1_in,
    l2_in,
    om_in,
    o1_in,
    o2_in,
    out_w,
    out_norm,
    lm_out,
    l1_out,
    l2_out,
    om_out,
    o1_out,
    o2_out,
    mine,
    other,
    sendbuf,
    recvbuf,
    wall,
    w32,
    obuf,
    lst,
    ost,
    tsum,
    dsum,
    tpart,
    dpart,
    load_sem,
    state_sem,
    store_sem,
    pair_s,
    pair_r,
    rs_s,
    rs_r,
    ag_s,
    ag_r,
    fw_s,
    fw_r,
    t_s,
    t_r,
    d_s,
    d_r,
):
    dp = lax.axis_index("dp")
    tn = lax.axis_index("tensor")
    core = lax.rem(dp, 2)
    chip = dp // 2
    chips = n // 2
    partner = chip * 2 + 1 - core
    rows, columns = mine.shape
    row_dev = rows // n
    kept = lst.shape[1]
    slots, off = ost.shape[1], ost.shape[2]
    width = columns // chunks
    pad = w32.shape[0]

    load = pltpu.make_async_copy(grads.at[0], mine, load_sem)
    load.start()
    loads = []
    for i, (ref, dst) in enumerate(
        zip((lm_in, l1_in, l2_in, om_in, o1_in, o2_in), [lst.at[i] for i in range(3)] + [ost.at[i] for i in range(3)])
    ):
        cp = pltpu.make_async_copy(ref, dst, state_sem.at[i])
        cp.start()
        loads.append(cp)

    barrier = pltpu.get_barrier_semaphore()

    def greet(k, c):
        pl.semaphore_signal(barrier, inc=1, device_id={"dp": lax.rem(dp + k, n)}, device_id_type=MESH)
        return c

    lax.fori_loop(1, n, greet, 0)
    for k in range(1, tensors):
        pl.semaphore_signal(barrier, inc=1, device_id={"tensor": lax.rem(tn + k, tensors)}, device_id_type=MESH)

    lane = lax.broadcasted_iota(jnp.int32, (1, rows), 1)
    sub = lax.broadcasted_iota(jnp.int32, (rows, 1), 0)

    def shard(s, carry):
        by_lane, by_sub, count = carry
        owner = owner_ref[s]
        count = count + jnp.where(owner == dp, 1, 0)

        def earlier(e, slot):
            return slot + jnp.where((owner_ref[e] == owner) & (e < s), 1, 0)

        slot = lax.fori_loop(0, n, earlier, 0)
        rank = jnp.int32(0)
        for j in range(row_dev):
            m = mask_ref[s, j]
            target = jnp.where(m == 1, owner * pad + kept + slot * off + rank, s * pad + (j - rank))
            rank = rank + m
            by_lane = jnp.where(lane == s * row_dev + j, target, by_lane)
            by_sub = jnp.where(sub == s * row_dev + j, target, by_sub)
        return by_lane, by_sub, count

    by_lane, by_sub, count = lax.fori_loop(
        0, n, shard, (jnp.zeros((1, rows), jnp.int32), jnp.zeros((rows, 1), jnp.int32), jnp.int32(0))
    )
    place = lax.broadcasted_iota(jnp.int32, (chips * pad, rows), 0)
    goal = (place // pad * 2 + core) * pad + place % pad
    route = jnp.where(goal == by_lane, 1.0, 0.0).astype(jnp.bfloat16)
    back = jnp.where(lax.broadcasted_iota(jnp.int32, (rows, n * pad), 1) == by_sub, 1.0, 0.0).astype(jnp.bfloat16)

    load.wait()
    pl.semaphore_wait(barrier, n - 1 + tensors - 1)

    pairs = []
    for c in range(chunks):
        cols = pl.ds(c * width, width)
        cp = pltpu.make_async_remote_copy(
            mine.at[:, cols], other.at[:, cols], pair_s.at[c], pair_r.at[c], device_id={"dp": partner}, device_id_type=MESH
        )
        cp.start()
        pairs.append(cp)

    scatter = []
    for c in range(chunks):
        cols = pl.ds(c * width, width)
        pairs[c].wait_recv()
        both = mine[:, cols].astype(jnp.float32) + other[:, cols].astype(jnp.float32)
        routed = jnp.dot(route, both.astype(jnp.bfloat16), preferred_element_type=jnp.float32)
        sendbuf[:, :, cols] = routed.reshape(chips, pad, width).astype(jnp.bfloat16)
        row = []
        for k in range(1, chips):
            to = lax.rem(chip + k, chips)
            cp = pltpu.make_async_remote_copy(
                sendbuf.at[to, :, cols],
                recvbuf.at[k - 1, :, cols],
                rs_s.at[k - 1, c],
                rs_r.at[k - 1, c],
                device_id={"dp": to * 2 + core},
                device_id_type=MESH,
            )
            cp.start()
            row.append(cp)
        scatter.append(row)

    for cp in loads:
        cp.wait()
    w32[...] = jnp.zeros_like(w32)
    squares = jnp.zeros((pad, LANES), jnp.float32)
    gather, own, stores = [], [], []
    for c in range(chunks):
        cols = pl.ds(c * width, width)
        total = sendbuf[chip, :, cols].astype(jnp.float32)
        for k in range(1, chips):
            scatter[c][k - 1].wait_recv()
            total = total + recvbuf[k - 1, :, cols].astype(jnp.float32)
        total = total / n
        sq = total * total
        for v in range(width // LANES):
            squares = squares + sq[:, v * LANES : (v + 1) * LANES]
        new = adam_update(lst[0, :, cols], lst[1, :, cols], lst[2, :, cols], total[:kept])
        for i in range(3):
            lst[i, :, cols] = new[i]
        w32[:kept, cols] = new[0]
        for s in range(slots):
            first = kept + s * off
            old = (ost[0, s, :, cols], ost[1, s, :, cols], ost[2, s, :, cols])
            new = adam_update(*old, total[first : first + off])
            filled = jnp.full(old[0].shape, count, jnp.int32) > s
            for i in range(3):
                value = jnp.where(filled, new[i], old[i])
                ost[i, s, :, cols] = value
                if i == 0:
                    w32[first : first + off, cols] = value
        wall[dp, :, cols] = w32[:, cols].astype(jnp.bfloat16)
        row = []
        for k in range(1, chips):
            to = lax.rem(chip + k, chips)
            cp = pltpu.make_async_remote_copy(
                wall.at[dp, :, cols],
                wall.at[dp, :, cols],
                ag_s.at[k - 1, c],
                ag_r.at[k - 1, c],
                device_id={"dp": to * 2 + core},
                device_id_type=MESH,
            )
            cp.start()
            row.append(cp)
        gather.append(row)
        cp = pltpu.make_async_remote_copy(
            wall.at[dp, :, cols],
            wall.at[dp, :, cols],
            fw_s.at[0, c],
            fw_r.at[0, c],
            device_id={"dp": partner},
            device_id_type=MESH,
        )
        cp.start()
        own.append(cp)

    for i, (ref, src) in enumerate(
        zip((lm_out, l1_out, l2_out, om_out, o1_out, o2_out), [lst.at[i] for i in range(3)] + [ost.at[i] for i in range(3)])
    ):
        cp = pltpu.make_async_copy(src, ref, state_sem.at[i])
        cp.start()
        stores.append(cp)

    tpart[...] = squares
    tcopies = []
    for k in range(1, tensors):
        cp = pltpu.make_async_remote_copy(
            tpart, tsum.at[k - 1], t_s.at[k - 1], t_r.at[k - 1], device_id={"tensor": lax.rem(tn + k, tensors)}, device_id_type=MESH
        )
        cp.start()
        tcopies.append(cp)
    for cp in tcopies:
        cp.wait()

    value = tpart[...]
    for k in range(1, tensors):
        value = value + tsum[k - 1]
    dpart[...] = value
    dcopies = []
    for k in range(1, n):
        cp = pltpu.make_async_remote_copy(
            dpart, dsum.at[k - 1], d_s.at[k - 1], d_r.at[k - 1], device_id={"dp": lax.rem(dp + k, n)}, device_id_type=MESH
        )
        cp.start()
        dcopies.append(cp)

    forwards = []
    for c in range(chunks):
        cols = pl.ds(c * width, width)
        row = [own[c]]
        for k in range(1, chips):
            gather[c][k - 1].wait_recv()
            src = lax.rem(chip + chips - k, chips) * 2 + core
            cp = pltpu.make_async_remote_copy(
                wall.at[src, :, cols],
                wall.at[src, :, cols],
                fw_s.at[k, c],
                fw_r.at[k, c],
                device_id={"dp": partner},
                device_id_type=MESH,
            )
            cp.start()
            row.append(cp)
        forwards.append(row)

    outs = []
    for c in range(chunks):
        cols = pl.ds(c * width, width)
        for cp in forwards[c]:
            cp.wait_recv()
        weights = wall[:, :, cols].reshape(n * pad, width)
        obuf[:, cols] = jnp.dot(back, weights, preferred_element_type=jnp.float32).astype(jnp.bfloat16)
        cp = pltpu.make_async_copy(obuf.at[:, cols], out_w.at[:, cols], store_sem.at[c])
        cp.start()
        outs.append(cp)

    value = dpart[...]
    for k in range(1, n):
        dcopies[k - 1].wait()
        value = value + dsum[k - 1]
    out_norm[...] = jnp.sqrt(jnp.sum(value, keepdims=True))

    for c in range(chunks):
        pairs[c].wait_send()
        for k in range(1, chips):
            scatter[c][k - 1].wait_send()
            gather[c][k - 1].wait_send()
        for cp in forwards[c]:
            cp.wait_send()
    for cp in stores:
        cp.wait()
    for cp in outs:
        cp.wait()


def body(n, tensors, grads, mask, owner, *states):
    rows, columns = grads.shape[1:]
    local, offload = states[0], states[3]
    chunks = 4
    while columns % (chunks * LANES):
        chunks -= 1
    chips = n // 2
    used = local.shape[0] + offload.shape[0] * offload.shape[1]
    pad = -(-used // SUBLANES) * SUBLANES
    any_space = pl.BlockSpec(memory_space=pl.ANY)
    smem = pl.BlockSpec(memory_space=pltpu.SMEM)
    dma = pltpu.SemaphoreType.DMA
    f32, bf16 = jnp.float32, jnp.bfloat16
    outs = pl.pallas_call(
        functools.partial(kernel, n, tensors, chunks),
        out_shape=[jax.ShapeDtypeStruct((rows, columns), bf16), jax.ShapeDtypeStruct((1, 1), f32)]
        + [jax.ShapeDtypeStruct(s.shape, f32) for s in states],
        in_specs=[smem, smem] + [any_space] * 7,
        out_specs=[any_space, pl.BlockSpec(memory_space=pltpu.VMEM)] + [any_space] * 6,
        scratch_shapes=[
            pltpu.VMEM((rows, columns), bf16),
            pltpu.VMEM((rows, columns), bf16),
            pltpu.VMEM((chips, pad, columns), bf16),
            pltpu.VMEM((chips - 1, pad, columns), bf16),
            pltpu.VMEM((n, pad, columns), bf16),
            pltpu.VMEM((pad, columns), f32),
            pltpu.VMEM((rows, columns), bf16),
            pltpu.VMEM((3,) + local.shape, f32),
            pltpu.VMEM((3,) + offload.shape, f32),
            pltpu.VMEM((tensors - 1, pad, LANES), f32),
            pltpu.VMEM((n - 1, pad, LANES), f32),
            pltpu.VMEM((pad, LANES), f32),
            pltpu.VMEM((pad, LANES), f32),
            dma,
            dma((6,)),
            dma((chunks,)),
            dma((chunks,)),
            dma((chunks,)),
            dma((chips - 1, chunks)),
            dma((chips - 1, chunks)),
            dma((chips - 1, chunks)),
            dma((chips - 1, chunks)),
            dma((chips, chunks)),
            dma((chips, chunks)),
            dma((tensors - 1,)),
            dma((tensors - 1,)),
            dma((n - 1,)),
            dma((n - 1,)),
        ],
        compiler_params=pltpu.CompilerParams(collective_id=0, has_side_effects=True),
        name="step",
    )(mask, owner, grads, *states)
    return (outs[0], outs[1][0, 0]) + tuple(outs[2:])


def solution(mesh):
    local, offload = P("dp", "tensor"), P("dp", None, "tensor")
    return jax.shard_map(
        functools.partial(body, mesh.shape["dp"], mesh.shape["tensor"]),
        mesh=mesh,
        in_specs=(P("dp", None, "tensor"), P(), P()) + (local,) * 3 + (offload,) * 3,
        out_specs=(P(None, "tensor"), P()) + (local,) * 3 + (offload,) * 3,
        check_vma=False,
    )
```

```python
import functools

import jax
import jax.numpy as jnp
from jax import lax
from jax.experimental import pallas as pl
from jax.experimental.pallas import tpu as pltpu
from jax.sharding import PartitionSpec as P

MESH = pl.DeviceIdType.MESH
beta_first = 0.9
beta_second = 0.95
learn_rate = 0.02
decay_rate = 0.1
epsilon_value = 1e-08
step_count = 10
bias_first = 1.0 - beta_first**step_count
bias_second = 1.0 - beta_second**step_count
LANES = 128
SUBLANES = 8
VMEM_BYTES = 67043328
ROOM = 8192


def adam_update(master, moment, second, gradient):
    moment_new = beta_first * moment + (1.0 - beta_first) * gradient
    second_new = beta_second * second + (1.0 - beta_second) * gradient * gradient
    scaled = moment_new / bias_first / (jnp.sqrt(second_new / bias_second) + epsilon_value)
    master_new = master - learn_rate * (scaled + decay_rate * master)
    return (master_new, moment_new, second_new)


def kernel(
    n,
    tensors,
    chunks,
    mask_ref,
    owner_ref,
    grads,
    lm_in,
    l1_in,
    l2_in,
    om_in,
    o1_in,
    o2_in,
    obuf,
    out_norm,
    lst,
    ost,
    mine,
    other,
    sendbuf,
    recvbuf,
    wall,
    w32,
    tsum,
    dsum,
    tpart,
    dpart,
    load_sem,
    state_sem,
    pair_s,
    pair_r,
    rs_s,
    rs_r,
    ag_s,
    ag_r,
    fw_s,
    fw_r,
    t_s,
    t_r,
    d_s,
    d_r,
):
    dp = lax.axis_index("dp")
    tn = lax.axis_index("tensor")
    core = lax.rem(dp, 2)
    chip = dp // 2
    chips = n // 2
    partner = chip * 2 + 1 - core
    rows, columns = mine.shape
    row_dev = rows // n
    kept = lst.shape[1]
    slots, off = ost.shape[1], ost.shape[2]
    width = columns // chunks
    pad = w32.shape[0]

    load = pltpu.make_async_copy(grads.at[0], mine, load_sem)
    load.start()
    loads = []
    for i, (ref, dst) in enumerate(
        zip((lm_in, l1_in, l2_in, om_in, o1_in, o2_in), [lst.at[i] for i in range(3)] + [ost.at[i] for i in range(3)])
    ):
        cp = pltpu.make_async_copy(ref, dst, state_sem.at[i])
        cp.start()
        loads.append(cp)

    barrier = pltpu.get_barrier_semaphore()

    def greet(k, c):
        pl.semaphore_signal(barrier, inc=1, device_id={"dp": lax.rem(dp + k, n)}, device_id_type=MESH)
        return c

    lax.fori_loop(1, n, greet, 0)
    for k in range(1, tensors):
        pl.semaphore_signal(barrier, inc=1, device_id={"tensor": lax.rem(tn + k, tensors)}, device_id_type=MESH)

    lane = lax.broadcasted_iota(jnp.int32, (1, rows), 1)
    sub = lax.broadcasted_iota(jnp.int32, (rows, 1), 0)

    def shard(s, carry):
        by_lane, by_sub, count = carry
        owner = owner_ref[s]
        count = count + jnp.where(owner == dp, 1, 0)

        def earlier(e, slot):
            return slot + jnp.where((owner_ref[e] == owner) & (e < s), 1, 0)

        slot = lax.fori_loop(0, n, earlier, 0)
        rank = jnp.int32(0)
        for j in range(row_dev):
            m = mask_ref[s, j]
            target = jnp.where(m == 1, owner * pad + kept + slot * off + rank, s * pad + (j - rank))
            rank = rank + m
            by_lane = jnp.where(lane == s * row_dev + j, target, by_lane)
            by_sub = jnp.where(sub == s * row_dev + j, target, by_sub)
        return by_lane, by_sub, count

    by_lane, by_sub, count = lax.fori_loop(
        0, n, shard, (jnp.zeros((1, rows), jnp.int32), jnp.zeros((rows, 1), jnp.int32), jnp.int32(0))
    )
    place = lax.broadcasted_iota(jnp.int32, (chips * pad, rows), 0)
    goal = (place // pad * 2 + core) * pad + place % pad
    route = jnp.where(goal == by_lane, 1.0, 0.0).astype(jnp.bfloat16)
    back = jnp.where(lax.broadcasted_iota(jnp.int32, (rows, n * pad), 1) == by_sub, 1.0, 0.0).astype(jnp.bfloat16)

    load.wait()
    pl.semaphore_wait(barrier, n - 1 + tensors - 1)

    pairs = []
    for c in range(chunks):
        cols = pl.ds(c * width, width)
        cp = pltpu.make_async_remote_copy(
            mine.at[:, cols], other.at[:, cols], pair_s.at[c], pair_r.at[c], device_id={"dp": partner}, device_id_type=MESH
        )
        cp.start()
        pairs.append(cp)

    scatter = []
    for c in range(chunks):
        cols = pl.ds(c * width, width)
        pairs[c].wait_recv()
        both = mine[:, cols].astype(jnp.float32) + other[:, cols].astype(jnp.float32)
        routed = jnp.dot(route, both.astype(jnp.bfloat16), preferred_element_type=jnp.float32)
        sendbuf[:, :, cols] = routed.reshape(chips, pad, width).astype(jnp.bfloat16)
        row = []
        for k in range(1, chips):
            to = lax.rem(chip + k, chips)
            cp = pltpu.make_async_remote_copy(
                sendbuf.at[to, :, cols],
                recvbuf.at[k - 1, :, cols],
                rs_s.at[k - 1, c],
                rs_r.at[k - 1, c],
                device_id={"dp": to * 2 + core},
                device_id_type=MESH,
            )
            cp.start()
            row.append(cp)
        scatter.append(row)

    for cp in loads:
        cp.wait()
    w32[...] = jnp.zeros_like(w32)
    squares = jnp.zeros((pad, LANES), jnp.float32)
    gather, own = [], []
    for c in range(chunks):
        cols = pl.ds(c * width, width)
        total = sendbuf[chip, :, cols].astype(jnp.float32)
        for k in range(1, chips):
            scatter[c][k - 1].wait_recv()
            total = total + recvbuf[k - 1, :, cols].astype(jnp.float32)
        total = total / n
        sq = total * total
        for v in range(width // LANES):
            squares = squares + sq[:, v * LANES : (v + 1) * LANES]
        new = adam_update(lst[0, :, cols], lst[1, :, cols], lst[2, :, cols], total[:kept])
        for i in range(3):
            lst[i, :, cols] = new[i]
        w32[:kept, cols] = new[0]
        for s in range(slots):
            first = kept + s * off
            old = (ost[0, s, :, cols], ost[1, s, :, cols], ost[2, s, :, cols])
            new = adam_update(*old, total[first : first + off])
            filled = jnp.full(old[0].shape, count, jnp.int32) > s
            for i in range(3):
                value = jnp.where(filled, new[i], old[i])
                ost[i, s, :, cols] = value
                if i == 0:
                    w32[first : first + off, cols] = value
        wall[dp, :, cols] = w32[:, cols].astype(jnp.bfloat16)
        row = []
        for k in range(1, chips):
            to = lax.rem(chip + k, chips)
            cp = pltpu.make_async_remote_copy(
                wall.at[dp, :, cols],
                wall.at[dp, :, cols],
                ag_s.at[k - 1, c],
                ag_r.at[k - 1, c],
                device_id={"dp": to * 2 + core},
                device_id_type=MESH,
            )
            cp.start()
            row.append(cp)
        gather.append(row)
        cp = pltpu.make_async_remote_copy(
            wall.at[dp, :, cols],
            wall.at[dp, :, cols],
            fw_s.at[0, c],
            fw_r.at[0, c],
            device_id={"dp": partner},
            device_id_type=MESH,
        )
        cp.start()
        own.append(cp)

    tpart[...] = squares
    tcopies = []
    for k in range(1, tensors):
        cp = pltpu.make_async_remote_copy(
            tpart, tsum.at[k - 1], t_s.at[k - 1], t_r.at[k - 1], device_id={"tensor": lax.rem(tn + k, tensors)}, device_id_type=MESH
        )
        cp.start()
        tcopies.append(cp)
    for cp in tcopies:
        cp.wait()

    value = tpart[...]
    for k in range(1, tensors):
        value = value + tsum[k - 1]
    dpart[...] = value
    dcopies = []
    for k in range(1, n):
        cp = pltpu.make_async_remote_copy(
            dpart, dsum.at[k - 1], d_s.at[k - 1], d_r.at[k - 1], device_id={"dp": lax.rem(dp + k, n)}, device_id_type=MESH
        )
        cp.start()
        dcopies.append(cp)

    forwards = []
    for c in range(chunks):
        cols = pl.ds(c * width, width)
        row = [own[c]]
        for k in range(1, chips):
            gather[c][k - 1].wait_recv()
            src = lax.rem(chip + chips - k, chips) * 2 + core
            cp = pltpu.make_async_remote_copy(
                wall.at[src, :, cols],
                wall.at[src, :, cols],
                fw_s.at[k, c],
                fw_r.at[k, c],
                device_id={"dp": partner},
                device_id_type=MESH,
            )
            cp.start()
            row.append(cp)
        forwards.append(row)

    for c in range(chunks):
        cols = pl.ds(c * width, width)
        for cp in forwards[c]:
            cp.wait_recv()
        weights = wall[:, :, cols].reshape(n * pad, width)
        obuf[:, cols] = jnp.dot(back, weights, preferred_element_type=jnp.float32).astype(jnp.bfloat16)

    value = dpart[...]
    for k in range(1, n):
        dcopies[k - 1].wait()
        value = value + dsum[k - 1]
    out_norm[...] = jnp.sqrt(jnp.sum(value, keepdims=True))

    for c in range(chunks):
        pairs[c].wait_send()
        for k in range(1, chips):
            scatter[c][k - 1].wait_send()
            gather[c][k - 1].wait_send()
        for cp in forwards[c]:
            cp.wait_send()


def store_kernel(weights, norm, new_local, new_offload, out_w, out_norm, *rest):
    outs, sem = rest[:6], rest[6]
    sources = [new_local.at[i] for i in range(3)] + [new_offload.at[i] for i in range(3)]
    copies = []
    for i, (src, dst) in enumerate(zip([weights] + sources, (out_w,) + outs)):
        cp = pltpu.make_async_copy(src, dst, sem.at[i])
        cp.start()
        copies.append(cp)
    out_norm[...] = norm[...]
    for cp in copies:
        cp.wait()


def body(n, tensors, grads, mask, owner, *states):
    rows, columns = grads.shape[1:]
    local, offload = states[0], states[3]
    chunks = 4
    while columns % (chunks * LANES):
        chunks -= 1
    chips = n // 2
    used = local.shape[0] + offload.shape[0] * offload.shape[1]
    pad = -(-used // SUBLANES) * SUBLANES
    kept_tile = -(-local.shape[0] // 4) * 4
    held = columns * (2 * rows + 12 * (kept_tile + offload.shape[0] * offload.shape[1]))
    limit = VMEM_BYTES - held - ROOM
    any_space = pl.BlockSpec(memory_space=pl.ANY)
    hbm = pl.BlockSpec(memory_space=pltpu.HBM)
    smem = pl.BlockSpec(memory_space=pltpu.SMEM)
    dma = pltpu.SemaphoreType.DMA
    f32, bf16 = jnp.float32, jnp.bfloat16
    vmem = pl.BlockSpec(memory_space=pltpu.VMEM)
    shapes = [((rows, columns), bf16), ((1, 1), f32), ((3,) + local.shape, f32), ((3,) + offload.shape, f32)]
    weights, norm, new_local, new_offload = pl.pallas_call(
        functools.partial(kernel, n, tensors, chunks),
        out_shape=[pltpu.VMEM(*s) for s in shapes],
        in_specs=[smem, smem] + [hbm] * 7,
        out_specs=[vmem] * 4,
        scratch_shapes=[
            pltpu.VMEM((rows, columns), bf16),
            pltpu.VMEM((rows, columns), bf16),
            pltpu.VMEM((chips, pad, columns), bf16),
            pltpu.VMEM((chips - 1, pad, columns), bf16),
            pltpu.VMEM((n, pad, columns), bf16),
            pltpu.VMEM((pad, columns), f32),
            pltpu.VMEM((tensors - 1, pad, LANES), f32),
            pltpu.VMEM((n - 1, pad, LANES), f32),
            pltpu.VMEM((pad, LANES), f32),
            pltpu.VMEM((pad, LANES), f32),
            dma,
            dma((6,)),
            dma((chunks,)),
            dma((chunks,)),
            dma((chips - 1, chunks)),
            dma((chips - 1, chunks)),
            dma((chips - 1, chunks)),
            dma((chips - 1, chunks)),
            dma((chips, chunks)),
            dma((chips, chunks)),
            dma((tensors - 1,)),
            dma((tensors - 1,)),
            dma((n - 1,)),
            dma((n - 1,)),
        ],
        compiler_params=pltpu.CompilerParams(
            collective_id=0, has_side_effects=True, vmem_limit_bytes=limit
        ),
        name="step",
    )(mask, owner, grads, *states)
    outs = pl.pallas_call(
        store_kernel,
        out_shape=[jax.ShapeDtypeStruct((rows, columns), bf16), jax.ShapeDtypeStruct((1, 1), f32)]
        + [jax.ShapeDtypeStruct(s.shape, f32) for s in states],
        in_specs=[any_space, vmem, any_space, any_space],
        out_specs=[any_space, vmem] + [any_space] * 6,
        scratch_shapes=[dma((7,))],
        compiler_params=pltpu.CompilerParams(vmem_limit_bytes=1 << 20),
        name="store",
    )(weights, norm, new_local, new_offload)
    return (outs[0], outs[1][0, 0]) + tuple(outs[2:])


def solution(mesh):
    local, offload = P("dp", "tensor"), P("dp", None, "tensor")
    return jax.shard_map(
        functools.partial(body, mesh.shape["dp"], mesh.shape["tensor"]),
        mesh=mesh,
        in_specs=(P("dp", None, "tensor"), P(), P()) + (local,) * 3 + (offload,) * 3,
        out_specs=(P(None, "tensor"), P()) + (local,) * 3 + (offload,) * 3,
        check_vma=False,
    )
```

```python
import functools

import jax
import jax.numpy as jnp
from jax import lax
from jax.experimental import pallas as pl
from jax.experimental.pallas import tpu as pltpu
from jax.sharding import PartitionSpec as P

MESH = pl.DeviceIdType.MESH
beta_first = 0.9
beta_second = 0.95
learn_rate = 0.02
decay_rate = 0.1
epsilon_value = 1e-08
step_count = 10
bias_first = 1.0 - beta_first**step_count
bias_second = 1.0 - beta_second**step_count
LANES = 128
SUBLANES = 8
VMEM_BYTES = 67043328
ROOM = 8192


def adam_update(master, moment, second, gradient):
    moment_new = beta_first * moment + (1.0 - beta_first) * gradient
    second_new = beta_second * second + (1.0 - beta_second) * gradient * gradient
    scaled = moment_new / bias_first / (jnp.sqrt(second_new / bias_second) + epsilon_value)
    master_new = master - learn_rate * (scaled + decay_rate * master)
    return (master_new, moment_new, second_new)


def kernel(
    n,
    tensors,
    chunks,
    mask_in,
    owner_in,
    grads,
    lm_in,
    l1_in,
    l2_in,
    om_in,
    o1_in,
    o2_in,
    obuf,
    out_norm,
    lst,
    ost,
    mask_ref,
    owner_ref,
    mine,
    other,
    sendbuf,
    recvbuf,
    wall,
    w32,
    tsum,
    dsum,
    tpart,
    dpart,
    load_sem,
    state_sem,
    table_sem,
    pair_s,
    pair_r,
    rs_s,
    rs_r,
    ag_s,
    ag_r,
    fw_s,
    fw_r,
    t_s,
    t_r,
    d_s,
    d_r,
):
    dp = lax.axis_index("dp")
    tn = lax.axis_index("tensor")
    core = lax.rem(dp, 2)
    chip = dp // 2
    chips = n // 2
    partner = chip * 2 + 1 - core
    rows, columns = mine.shape
    row_dev = rows // n
    kept = lst.shape[1]
    slots, off = ost.shape[1], ost.shape[2]
    width = columns // chunks
    pad = w32.shape[0]

    barrier = pltpu.get_barrier_semaphore()

    def greet(k, c):
        pl.semaphore_signal(barrier, inc=1, device_id={"dp": lax.rem(dp + k, n)}, device_id_type=MESH)
        return c

    lax.fori_loop(1, n, greet, 0)
    for k in range(1, tensors):
        pl.semaphore_signal(barrier, inc=1, device_id={"tensor": lax.rem(tn + k, tensors)}, device_id_type=MESH)

    load = pltpu.make_async_copy(grads.at[0], mine, load_sem)
    load.start()
    tables = []
    for i, (ref, dst) in enumerate(((mask_in, mask_ref), (owner_in, owner_ref))):
        cp = pltpu.make_async_copy(ref, dst, table_sem.at[i])
        cp.start()
        tables.append(cp)
    loads = []
    for i, (ref, dst) in enumerate(
        zip((lm_in, l1_in, l2_in, om_in, o1_in, o2_in), [lst.at[i] for i in range(3)] + [ost.at[i] for i in range(3)])
    ):
        cp = pltpu.make_async_copy(ref, dst, state_sem.at[i])
        cp.start()
        loads.append(cp)

    for cp in tables:
        cp.wait()
    lane = lax.broadcasted_iota(jnp.int32, (1, rows), 1)
    sub = lax.broadcasted_iota(jnp.int32, (rows, 1), 0)

    def shard(s, carry):
        by_lane, by_sub, count = carry
        owner = owner_ref[s]
        count = count + jnp.where(owner == dp, 1, 0)

        def earlier(e, slot):
            return slot + jnp.where((owner_ref[e] == owner) & (e < s), 1, 0)

        slot = lax.fori_loop(0, n, earlier, 0)
        rank = jnp.int32(0)
        for j in range(row_dev):
            m = mask_ref[s, j]
            target = jnp.where(m == 1, owner * pad + kept + slot * off + rank, s * pad + (j - rank))
            rank = rank + m
            by_lane = jnp.where(lane == s * row_dev + j, target, by_lane)
            by_sub = jnp.where(sub == s * row_dev + j, target, by_sub)
        return by_lane, by_sub, count

    by_lane, by_sub, count = lax.fori_loop(
        0, n, shard, (jnp.zeros((1, rows), jnp.int32), jnp.zeros((rows, 1), jnp.int32), jnp.int32(0))
    )
    place = lax.broadcasted_iota(jnp.int32, (chips * pad, rows), 0)
    goal = (place // pad * 2 + core) * pad + place % pad
    route = jnp.where(goal == by_lane, 1.0, 0.0).astype(jnp.bfloat16)
    back = jnp.where(lax.broadcasted_iota(jnp.int32, (rows, n * pad), 1) == by_sub, 1.0, 0.0).astype(jnp.bfloat16)

    load.wait()
    pl.semaphore_wait(barrier, n - 1 + tensors - 1)

    pairs = []
    for c in range(chunks):
        cols = pl.ds(c * width, width)
        cp = pltpu.make_async_remote_copy(
            mine.at[:, cols], other.at[:, cols], pair_s.at[c], pair_r.at[c], device_id={"dp": partner}, device_id_type=MESH
        )
        cp.start()
        pairs.append(cp)

    scatter = []
    for c in range(chunks):
        cols = pl.ds(c * width, width)
        pairs[c].wait_recv()
        both = mine[:, cols].astype(jnp.float32) + other[:, cols].astype(jnp.float32)
        routed = jnp.dot(route, both.astype(jnp.bfloat16), preferred_element_type=jnp.float32)
        sendbuf[:, :, cols] = routed.reshape(chips, pad, width).astype(jnp.bfloat16)
        row = []
        for k in range(1, chips):
            to = lax.rem(chip + k, chips)
            cp = pltpu.make_async_remote_copy(
                sendbuf.at[to, :, cols],
                recvbuf.at[k - 1, :, cols],
                rs_s.at[k - 1, c],
                rs_r.at[k - 1, c],
                device_id={"dp": to * 2 + core},
                device_id_type=MESH,
            )
            cp.start()
            row.append(cp)
        scatter.append(row)

    for cp in loads:
        cp.wait()
    w32[...] = jnp.zeros_like(w32)
    squares = jnp.zeros((pad, LANES), jnp.float32)
    gather, own = [], []
    for c in range(chunks):
        cols = pl.ds(c * width, width)
        total = sendbuf[chip, :, cols].astype(jnp.float32)
        for k in range(1, chips):
            scatter[c][k - 1].wait_recv()
            total = total + recvbuf[k - 1, :, cols].astype(jnp.float32)
        total = total / n
        sq = total * total
        for v in range(width // LANES):
            squares = squares + sq[:, v * LANES : (v + 1) * LANES]
        new = adam_update(lst[0, :, cols], lst[1, :, cols], lst[2, :, cols], total[:kept])
        for i in range(3):
            lst[i, :, cols] = new[i]
        w32[:kept, cols] = new[0]
        for s in range(slots):
            first = kept + s * off
            old = (ost[0, s, :, cols], ost[1, s, :, cols], ost[2, s, :, cols])
            new = adam_update(*old, total[first : first + off])
            filled = jnp.full(old[0].shape, count, jnp.int32) > s
            for i in range(3):
                value = jnp.where(filled, new[i], old[i])
                ost[i, s, :, cols] = value
                if i == 0:
                    w32[first : first + off, cols] = value
        wall[dp, :, cols] = w32[:, cols].astype(jnp.bfloat16)
        row = []
        for k in range(1, chips):
            to = lax.rem(chip + k, chips)
            cp = pltpu.make_async_remote_copy(
                wall.at[dp, :, cols],
                wall.at[dp, :, cols],
                ag_s.at[k - 1, c],
                ag_r.at[k - 1, c],
                device_id={"dp": to * 2 + core},
                device_id_type=MESH,
            )
            cp.start()
            row.append(cp)
        gather.append(row)
        cp = pltpu.make_async_remote_copy(
            wall.at[dp, :, cols],
            wall.at[dp, :, cols],
            fw_s.at[0, c],
            fw_r.at[0, c],
            device_id={"dp": partner},
            device_id_type=MESH,
        )
        cp.start()
        own.append(cp)

    tpart[...] = squares
    tcopies = []
    for k in range(1, tensors):
        cp = pltpu.make_async_remote_copy(
            tpart, tsum.at[k - 1], t_s.at[k - 1], t_r.at[k - 1], device_id={"tensor": lax.rem(tn + k, tensors)}, device_id_type=MESH
        )
        cp.start()
        tcopies.append(cp)
    forwards = []
    for c in range(chunks):
        cols = pl.ds(c * width, width)
        if c == chunks - 1:
            for cp in tcopies:
                cp.wait()
            value = tpart[...]
            for k in range(1, tensors):
                value = value + tsum[k - 1]
            dpart[...] = value
            dcopies = []
            for k in range(1, n):
                cp = pltpu.make_async_remote_copy(
                    dpart, dsum.at[k - 1], d_s.at[k - 1], d_r.at[k - 1], device_id={"dp": lax.rem(dp + k, n)}, device_id_type=MESH
                )
                cp.start()
                dcopies.append(cp)
        row = [own[c]]
        for k in range(1, chips):
            gather[c][k - 1].wait_recv()
            src = lax.rem(chip + chips - k, chips) * 2 + core
            cp = pltpu.make_async_remote_copy(
                wall.at[src, :, cols],
                wall.at[src, :, cols],
                fw_s.at[k, c],
                fw_r.at[k, c],
                device_id={"dp": partner},
                device_id_type=MESH,
            )
            cp.start()
            row.append(cp)
        forwards.append(row)

    for c in range(chunks):
        cols = pl.ds(c * width, width)
        for cp in forwards[c]:
            cp.wait_recv()
        weights = wall[:, :, cols].reshape(n * pad, width)
        obuf[:, cols] = jnp.dot(back, weights, preferred_element_type=jnp.float32).astype(jnp.bfloat16)

    value = dpart[...]
    for k in range(1, n):
        dcopies[k - 1].wait()
        value = value + dsum[k - 1]
    out_norm[...] = jnp.sqrt(jnp.sum(value, keepdims=True))

    for c in range(chunks):
        pairs[c].wait_send()
        for k in range(1, chips):
            scatter[c][k - 1].wait_send()
            gather[c][k - 1].wait_send()
        for cp in forwards[c]:
            cp.wait_send()


def store_kernel(weights, norm, new_local, new_offload, out_w, out_norm, *rest):
    outs, sem = rest[:6], rest[6]
    sources = [new_local.at[i] for i in range(3)] + [new_offload.at[i] for i in range(3)]
    copies = []
    for i, (src, dst) in enumerate(zip([weights] + sources, (out_w,) + outs)):
        cp = pltpu.make_async_copy(src, dst, sem.at[i])
        cp.start()
        copies.append(cp)
    out_norm[...] = norm[...]
    for cp in copies:
        cp.wait()


def body(n, tensors, grads, mask, owner, *states):
    rows, columns = grads.shape[1:]
    local, offload = states[0], states[3]
    chunks = 4
    while columns % (chunks * LANES):
        chunks -= 1
    chips = n // 2
    used = local.shape[0] + offload.shape[0] * offload.shape[1]
    pad = -(-used // SUBLANES) * SUBLANES
    kept_tile = -(-local.shape[0] // 4) * 4
    held = columns * (2 * rows + 12 * (kept_tile + offload.shape[0] * offload.shape[1]))
    limit = VMEM_BYTES - held - ROOM
    any_space = pl.BlockSpec(memory_space=pl.ANY)
    hbm = pl.BlockSpec(memory_space=pltpu.HBM)
    dma = pltpu.SemaphoreType.DMA
    f32, bf16 = jnp.float32, jnp.bfloat16
    vmem = pl.BlockSpec(memory_space=pltpu.VMEM)
    shapes = [((rows, columns), bf16), ((1, 1), f32), ((3,) + local.shape, f32), ((3,) + offload.shape, f32)]
    weights, norm, new_local, new_offload = pl.pallas_call(
        functools.partial(kernel, n, tensors, chunks),
        out_shape=[pltpu.VMEM(*s) for s in shapes],
        in_specs=[hbm] * 9,
        out_specs=[vmem] * 4,
        scratch_shapes=[
            pltpu.SMEM(mask.shape, jnp.int32),
            pltpu.SMEM(owner.shape, jnp.int32),
            pltpu.VMEM((rows, columns), bf16),
            pltpu.VMEM((rows, columns), bf16),
            pltpu.VMEM((chips, pad, columns), bf16),
            pltpu.VMEM((chips - 1, pad, columns), bf16),
            pltpu.VMEM((n, pad, columns), bf16),
            pltpu.VMEM((pad, columns), f32),
            pltpu.VMEM((tensors - 1, pad, LANES), f32),
            pltpu.VMEM((n - 1, pad, LANES), f32),
            pltpu.VMEM((pad, LANES), f32),
            pltpu.VMEM((pad, LANES), f32),
            dma,
            dma((6,)),
            dma((2,)),
            dma((chunks,)),
            dma((chunks,)),
            dma((chips - 1, chunks)),
            dma((chips - 1, chunks)),
            dma((chips - 1, chunks)),
            dma((chips - 1, chunks)),
            dma((chips, chunks)),
            dma((chips, chunks)),
            dma((tensors - 1,)),
            dma((tensors - 1,)),
            dma((n - 1,)),
            dma((n - 1,)),
        ],
        compiler_params=pltpu.CompilerParams(
            collective_id=0, has_side_effects=True, vmem_limit_bytes=limit
        ),
        name="step",
    )(mask, owner, grads, *states)
    outs = pl.pallas_call(
        store_kernel,
        out_shape=[jax.ShapeDtypeStruct((rows, columns), bf16), jax.ShapeDtypeStruct((1, 1), f32)]
        + [jax.ShapeDtypeStruct(s.shape, f32) for s in states],
        in_specs=[any_space, vmem, any_space, any_space],
        out_specs=[any_space, vmem] + [any_space] * 6,
        scratch_shapes=[dma((7,))],
        compiler_params=pltpu.CompilerParams(vmem_limit_bytes=1 << 20),
        name="store",
    )(weights, norm, new_local, new_offload)
    return (outs[0], outs[1][0, 0]) + tuple(outs[2:])


def solution(mesh):
    local, offload = P("dp", "tensor"), P("dp", None, "tensor")
    return jax.shard_map(
        functools.partial(body, mesh.shape["dp"], mesh.shape["tensor"]),
        mesh=mesh,
        in_specs=(P("dp", None, "tensor"), P(), P()) + (local,) * 3 + (offload,) * 3,
        out_specs=(P(None, "tensor"), P()) + (local,) * 3 + (offload,) * 3,
        check_vma=False,
    )
```

```python
import functools

import jax
import jax.numpy as jnp
from jax import lax
from jax.experimental import pallas as pl
from jax.experimental.pallas import tpu as pltpu
from jax.sharding import PartitionSpec as P

MESH = pl.DeviceIdType.MESH
beta_first = 0.9
beta_second = 0.95
learn_rate = 0.02
decay_rate = 0.1
epsilon_value = 1e-08
step_count = 10
bias_first = 1.0 - beta_first**step_count
bias_second = 1.0 - beta_second**step_count
LANES = 128
SUBLANES = 8
VMEM_BYTES = 67043328
ROOM = 8192


def adam_update(master, moment, second, gradient):
    moment_new = beta_first * moment + (1.0 - beta_first) * gradient
    second_new = beta_second * second + (1.0 - beta_second) * gradient * gradient
    scaled = moment_new / bias_first / (jnp.sqrt(second_new / bias_second) + epsilon_value)
    master_new = master - learn_rate * (scaled + decay_rate * master)
    return (master_new, moment_new, second_new)


def kernel(
    n,
    tensors,
    chunks,
    mask_in,
    owner_in,
    grads,
    lm_in,
    l1_in,
    l2_in,
    om_in,
    o1_in,
    o2_in,
    obuf,
    out_norm,
    lst,
    ost,
    mask_ref,
    owner_ref,
    mine,
    other,
    sendbuf,
    recvbuf,
    wall,
    w32,
    tsum,
    dsum,
    tpart,
    dpart,
    load_sem,
    state_sem,
    table_sem,
    pair_s,
    pair_r,
    rs_s,
    rs_r,
    ag_s,
    ag_r,
    fw_s,
    fw_r,
    t_s,
    t_r,
    d_s,
    d_r,
):
    dp = lax.axis_index("dp")
    tn = lax.axis_index("tensor")
    core = lax.rem(dp, 2)
    chip = dp // 2
    chips = n // 2
    partner = chip * 2 + 1 - core
    rows, columns = mine.shape
    row_dev = rows // n
    kept = lst.shape[1]
    slots, off = ost.shape[1], ost.shape[2]
    width = columns // chunks
    pad = w32.shape[0]

    def peer(k):
        return sum((chip // b + k // b) % 2 * b for b in bits)

    bits = [1 << i for i in range(chips.bit_length() - 1)]
    order = sorted(range(1, chips), key=lambda k: -bin(k).count("1"))
    barrier = pltpu.get_barrier_semaphore()

    def greet(k, c):
        pl.semaphore_signal(barrier, inc=1, device_id={"dp": lax.rem(dp + k, n)}, device_id_type=MESH)
        return c

    for k in range(1, tensors):
        pl.semaphore_signal(barrier, inc=1, device_id={"tensor": lax.rem(tn + k, tensors)}, device_id_type=MESH)
    lax.fori_loop(1, n, greet, 0)

    load = pltpu.make_async_copy(grads.at[0], mine, load_sem)
    load.start()
    tables = []
    for i, (ref, dst) in enumerate(((mask_in, mask_ref), (owner_in, owner_ref))):
        cp = pltpu.make_async_copy(ref, dst, table_sem.at[i])
        cp.start()
        tables.append(cp)
    loads = []
    for i, (ref, dst) in enumerate(
        zip((lm_in, l1_in, l2_in, om_in, o1_in, o2_in), [lst.at[i] for i in range(3)] + [ost.at[i] for i in range(3)])
    ):
        cp = pltpu.make_async_copy(ref, dst, state_sem.at[i])
        cp.start()
        loads.append(cp)

    for cp in tables:
        cp.wait()
    lane = lax.broadcasted_iota(jnp.int32, (1, rows), 1)
    sub = lax.broadcasted_iota(jnp.int32, (rows, 1), 0)

    def shard(s, carry):
        by_lane, by_sub, count = carry
        owner = owner_ref[s]
        count = count + jnp.where(owner == dp, 1, 0)

        def earlier(e, slot):
            return slot + jnp.where((owner_ref[e] == owner) & (e < s), 1, 0)

        slot = lax.fori_loop(0, n, earlier, 0)
        rank = jnp.int32(0)
        for j in range(row_dev):
            m = mask_ref[s, j]
            target = jnp.where(m == 1, owner * pad + kept + slot * off + rank, s * pad + (j - rank))
            rank = rank + m
            by_lane = jnp.where(lane == s * row_dev + j, target, by_lane)
            by_sub = jnp.where(sub == s * row_dev + j, target, by_sub)
        return by_lane, by_sub, count

    by_lane, by_sub, count = lax.fori_loop(
        0, n, shard, (jnp.zeros((1, rows), jnp.int32), jnp.zeros((rows, 1), jnp.int32), jnp.int32(0))
    )
    place = lax.broadcasted_iota(jnp.int32, (chips * pad, rows), 0)
    goal = (place // pad * 2 + core) * pad + place % pad
    route = jnp.where(goal == by_lane, 1.0, 0.0).astype(jnp.bfloat16)
    back = jnp.where(lax.broadcasted_iota(jnp.int32, (rows, n * pad), 1) == by_sub, 1.0, 0.0).astype(jnp.bfloat16)

    load.wait()
    pl.semaphore_wait(barrier, n - 1 + tensors - 1)

    pairs = []
    for c in range(chunks):
        cols = pl.ds(c * width, width)
        cp = pltpu.make_async_remote_copy(
            mine.at[:, cols], other.at[:, cols], pair_s.at[c], pair_r.at[c], device_id={"dp": partner}, device_id_type=MESH
        )
        cp.start()
        pairs.append(cp)

    scatter = []
    for c in range(chunks):
        cols = pl.ds(c * width, width)
        pairs[c].wait_recv()
        both = mine[:, cols].astype(jnp.float32) + other[:, cols].astype(jnp.float32)
        routed = jnp.dot(route, both.astype(jnp.bfloat16), preferred_element_type=jnp.float32)
        sendbuf[:, :, cols] = routed.reshape(chips, pad, width).astype(jnp.bfloat16)
        row = {}
        for k in order:
            to = peer(k)
            cp = pltpu.make_async_remote_copy(
                sendbuf.at[to, :, cols],
                recvbuf.at[k - 1, :, cols],
                rs_s.at[k - 1, c],
                rs_r.at[k - 1, c],
                device_id={"dp": to * 2 + core},
                device_id_type=MESH,
            )
            cp.start()
            row[k] = cp
        scatter.append(row)

    for cp in loads:
        cp.wait()
    w32[...] = jnp.zeros_like(w32)
    squares = jnp.zeros((pad, LANES), jnp.float32)
    gather, own = [], []
    for c in range(chunks):
        cols = pl.ds(c * width, width)
        total = sendbuf[chip, :, cols].astype(jnp.float32)
        for k in range(1, chips):
            scatter[c][k].wait_recv()
            total = total + recvbuf[k - 1, :, cols].astype(jnp.float32)
        total = total / n
        sq = total * total
        for v in range(width // LANES):
            squares = squares + sq[:, v * LANES : (v + 1) * LANES]
        if c == chunks - 1:
            tpart[...] = squares
            tcopies = []
            for k in range(1, tensors):
                cp = pltpu.make_async_remote_copy(
                    tpart, tsum.at[k - 1], t_s.at[k - 1], t_r.at[k - 1], device_id={"tensor": lax.rem(tn + k, tensors)}, device_id_type=MESH
                )
                cp.start()
                tcopies.append(cp)
        new = adam_update(lst[0, :, cols], lst[1, :, cols], lst[2, :, cols], total[:kept])
        for i in range(3):
            lst[i, :, cols] = new[i]
        w32[:kept, cols] = new[0]
        for s in range(slots):
            first = kept + s * off
            old = (ost[0, s, :, cols], ost[1, s, :, cols], ost[2, s, :, cols])
            new = adam_update(*old, total[first : first + off])
            filled = jnp.full(old[0].shape, count, jnp.int32) > s
            for i in range(3):
                value = jnp.where(filled, new[i], old[i])
                ost[i, s, :, cols] = value
                if i == 0:
                    w32[first : first + off, cols] = value
        wall[dp, :, cols] = w32[:, cols].astype(jnp.bfloat16)
        row = {}
        for k in order:
            to = peer(k)
            cp = pltpu.make_async_remote_copy(
                wall.at[dp, :, cols],
                wall.at[dp, :, cols],
                ag_s.at[k - 1, c],
                ag_r.at[k - 1, c],
                device_id={"dp": to * 2 + core},
                device_id_type=MESH,
            )
            cp.start()
            row[k] = cp
        gather.append(row)
        cp = pltpu.make_async_remote_copy(
            wall.at[dp, :, cols],
            wall.at[dp, :, cols],
            fw_s.at[0, c],
            fw_r.at[0, c],
            device_id={"dp": partner},
            device_id_type=MESH,
        )
        cp.start()
        own.append(cp)

    forwards = []
    for c in range(chunks):
        cols = pl.ds(c * width, width)
        if c == chunks - 1:
            for cp in tcopies:
                cp.wait()
            value = tpart[...]
            for k in range(1, tensors):
                value = value + tsum[k - 1]
            dpart[...] = value
            dcopies = []
            for k in range(1, n):
                cp = pltpu.make_async_remote_copy(
                    dpart, dsum.at[k - 1], d_s.at[k - 1], d_r.at[k - 1], device_id={"dp": lax.rem(dp + k, n)}, device_id_type=MESH
                )
                cp.start()
                dcopies.append(cp)
        row = [own[c]]
        for k in range(1, chips):
            gather[c][k].wait_recv()
            src = peer(k) * 2 + core
            cp = pltpu.make_async_remote_copy(
                wall.at[src, :, cols],
                wall.at[src, :, cols],
                fw_s.at[k, c],
                fw_r.at[k, c],
                device_id={"dp": partner},
                device_id_type=MESH,
            )
            cp.start()
            row.append(cp)
        forwards.append(row)

    for c in range(chunks):
        cols = pl.ds(c * width, width)
        for cp in forwards[c]:
            cp.wait_recv()
        weights = wall[:, :, cols].reshape(n * pad, width)
        obuf[:, cols] = jnp.dot(back, weights, preferred_element_type=jnp.float32).astype(jnp.bfloat16)

    value = dpart[...]
    for k in range(1, n):
        dcopies[k - 1].wait()
        value = value + dsum[k - 1]
    out_norm[...] = jnp.sqrt(jnp.sum(value, keepdims=True))

    for c in range(chunks):
        pairs[c].wait_send()
        for k in range(1, chips):
            scatter[c][k].wait_send()
            gather[c][k].wait_send()
        for cp in forwards[c]:
            cp.wait_send()


def store_kernel(weights, norm, new_local, new_offload, out_w, out_norm, *rest):
    outs, sem = rest[:6], rest[6]
    sources = [new_local.at[i] for i in range(3)] + [new_offload.at[i] for i in range(3)]
    copies = []
    for i, (src, dst) in enumerate(zip([weights] + sources, (out_w,) + outs)):
        cp = pltpu.make_async_copy(src, dst, sem.at[i])
        cp.start()
        copies.append(cp)
    out_norm[...] = norm[...]
    for cp in copies:
        cp.wait()


def body(n, tensors, grads, mask, owner, *states):
    rows, columns = grads.shape[1:]
    local, offload = states[0], states[3]
    chunks = 2
    while columns % (chunks * LANES):
        chunks -= 1
    chips = n // 2
    used = local.shape[0] + offload.shape[0] * offload.shape[1]
    pad = -(-used // SUBLANES) * SUBLANES
    kept_tile = -(-local.shape[0] // 4) * 4
    held = columns * (2 * rows + 12 * (kept_tile + offload.shape[0] * offload.shape[1]))
    limit = VMEM_BYTES - held - ROOM
    any_space = pl.BlockSpec(memory_space=pl.ANY)
    hbm = pl.BlockSpec(memory_space=pltpu.HBM)
    dma = pltpu.SemaphoreType.DMA
    f32, bf16 = jnp.float32, jnp.bfloat16
    vmem = pl.BlockSpec(memory_space=pltpu.VMEM)
    shapes = [((rows, columns), bf16), ((1, 1), f32), ((3,) + local.shape, f32), ((3,) + offload.shape, f32)]
    weights, norm, new_local, new_offload = pl.pallas_call(
        functools.partial(kernel, n, tensors, chunks),
        out_shape=[pltpu.VMEM(*s) for s in shapes],
        in_specs=[hbm] * 9,
        out_specs=[vmem] * 4,
        scratch_shapes=[
            pltpu.SMEM(mask.shape, jnp.int32),
            pltpu.SMEM(owner.shape, jnp.int32),
            pltpu.VMEM((rows, columns), bf16),
            pltpu.VMEM((rows, columns), bf16),
            pltpu.VMEM((chips, pad, columns), bf16),
            pltpu.VMEM((chips - 1, pad, columns), bf16),
            pltpu.VMEM((n, pad, columns), bf16),
            pltpu.VMEM((pad, columns), f32),
            pltpu.VMEM((tensors - 1, pad, LANES), f32),
            pltpu.VMEM((n - 1, pad, LANES), f32),
            pltpu.VMEM((pad, LANES), f32),
            pltpu.VMEM((pad, LANES), f32),
            dma,
            dma((6,)),
            dma((2,)),
            dma((chunks,)),
            dma((chunks,)),
            dma((chips - 1, chunks)),
            dma((chips - 1, chunks)),
            dma((chips - 1, chunks)),
            dma((chips - 1, chunks)),
            dma((chips, chunks)),
            dma((chips, chunks)),
            dma((tensors - 1,)),
            dma((tensors - 1,)),
            dma((n - 1,)),
            dma((n - 1,)),
        ],
        compiler_params=pltpu.CompilerParams(
            collective_id=0, has_side_effects=True, vmem_limit_bytes=limit
        ),
        name="step",
    )(mask, owner, grads, *states)
    outs = pl.pallas_call(
        store_kernel,
        out_shape=[jax.ShapeDtypeStruct((rows, columns), bf16), jax.ShapeDtypeStruct((1, 1), f32)]
        + [jax.ShapeDtypeStruct(s.shape, f32) for s in states],
        in_specs=[any_space, vmem, any_space, any_space],
        out_specs=[any_space, vmem] + [any_space] * 6,
        scratch_shapes=[dma((7,))],
        compiler_params=pltpu.CompilerParams(vmem_limit_bytes=1 << 20),
        name="store",
    )(weights, norm, new_local, new_offload)
    return (outs[0], outs[1][0, 0]) + tuple(outs[2:])


def solution(mesh):
    local, offload = P("dp", "tensor"), P("dp", None, "tensor")
    return jax.shard_map(
        functools.partial(body, mesh.shape["dp"], mesh.shape["tensor"]),
        mesh=mesh,
        in_specs=(P("dp", None, "tensor"), P(), P()) + (local,) * 3 + (offload,) * 3,
        out_specs=(P(None, "tensor"), P()) + (local,) * 3 + (offload,) * 3,
        check_vma=False,
    )
```
